32 devices in a mesh: row: 4 (over x, core), col: 8 (over z, y).
Axes of the slice: x: 2, y: 2, z: 4, core: 2. Of those that a mesh axis runs over, the one named last changes fastest.
Arguments:
- pooled: bfloat16 [2048, 1152], P(('row', 'col')), may hold values from -32 to 32
- hidden: bfloat16 [2048, 4304], P(('row', 'col')), may hold values from -6 to 6
- text: bfloat16 [2048, 1152], P(('row', 'col')), may hold values from -12 to 12
- weight: float32 [1152, 4304], P('col', 'row'), may hold values from -0.09375 to 0.09375
- row_moment: float32 [1152], P('col'), may hold values from 1e-07 to 1e-05
- col_moment: float32 [4304], P('row'), may hold values from 1e-07 to 1e-05
- log_scale: float32 [], replicated, may hold values from 4.2 to 4.8
- bias: float32 [], replicated, may hold values from -16 to -12
Outputs:
- update: float32 [1152, 4304], P('col', 'row')
- new_row: float32 [1152], P('col')
- new_col: float32 [4304], P('row')
- loss: float32 [], replicated
The draws below stay inside these ranges and needn't reach their ends.
All inputs are finite; a program needn't handle non-finite values.
Results may differ from the reference program's by a relative error of at most 0.004.
Values may be sent and summed in bfloat16 or wider, within the bound.
A program may use at most 128 MiB of HBM per device.

```python
import math
import jax
import jax.numpy as jnp
from jax import lax

D = 1152
FF = 4304
TOK_DEV = 64
BATCH = 2048
N_ROW = 4
N_COL = 8


def noise_block(key, shape):
    return jax.random.normal(key, shape, jnp.float32)


def pair_parts(key):
    folded = jax.random.fold_in(key, 4242)
    subkeys = jax.random.split(folded, 6)
    group_count = 16
    centers = noise_block(subkeys[0], (group_count, D))
    members = jax.random.randint(subkeys[1], (BATCH,), 0, group_count)
    onehot = (members[:, None] == jnp.arange(group_count, dtype=jnp.int32)[None, :]).astype(jnp.float32)
    cluster = jnp.dot(onehot, centers, precision=lax.Precision.HIGHEST)
    shared = noise_block(subkeys[2], (BATCH, D))
    strength = jax.random.uniform(subkeys[3], (BATCH, 1), jnp.float32, 0.1, 0.5)
    own_image = noise_block(subkeys[4], (BATCH, D))
    own_text = noise_block(subkeys[5], (BATCH, D))
    cluster_weight = 0.5
    image_side = cluster_weight * cluster + shared + 1.5 * own_image
    text_side = cluster_weight * cluster + strength * shared + 1.5 * own_text
    return (jnp.clip(image_side, -32.0, 32.0), jnp.clip(text_side, -12.0, 12.0))


def draw_pooled(key, part):
    return pair_parts(key)[0].astype(jnp.bfloat16)


def draw_text(key, part):
    return pair_parts(key)[1].astype(jnp.bfloat16)


def block_levels(key, extent, cuts, least, largest):
    loudness, own = 1.0, jax.random.fold_in(key, 6)
    for axis_at, shards_of in cuts:
        heights = jnp.exp(jax.random.uniform(jax.random.fold_in(own, axis_at), (shards_of,), jnp.float32, least / len(cuts), largest / len(cuts)))
        loudness = loudness * jnp.repeat(heights, extent[axis_at] // shards_of).reshape([-1 if axis == axis_at else 1 for axis in range(len(extent))])
    return loudness


def scatter_about(key, shape, spread, bound, cuts=(), kind=jnp.bfloat16):
    array = jax.random.normal(key, shape, jnp.float32) * spread
    if len(cuts) > 0:
        array = block_levels(key, shape, cuts, -0.22, 0.18) * array
    return jnp.clip(array, min=-bound, max=bound).astype(kind)


def setup_inputs(seed: int = 0) -> dict:
    streams_of = jax.random.split(jax.random.key(seed), 9)
    pooled = draw_pooled(jax.random.fold_in(streams_of[8], 71), 0)
    hidden = scatter_about(streams_of[1], (BATCH, FF), 1.0, 6.0, ((0, 32),))
    text = draw_text(jax.random.fold_in(streams_of[8], 71), 0)
    weight = scatter_about(streams_of[3], (D, FF), FF ** -0.5, 0.09375, ((0, 8), (1, 4)), jnp.float32)
    row_moment = jnp.clip(jnp.exp(math.log(9.999999747378752e-06) - 4.6051701 * jax.random.uniform(streams_of[4], (D,), jnp.float32) ** block_levels(streams_of[4], (D,), ((0, 8),), -0.2, 0.2)), 1.0000000116860974e-07, 9.999999747378752e-06)
    col_moment = jnp.clip(jnp.exp(math.log(9.999999747378752e-06) - 4.6051701 * jax.random.uniform(streams_of[5], (FF,), jnp.float32) ** block_levels(streams_of[5], (FF,), ((0, 4),), -0.2, 0.2)), 1.0000000116860974e-07, 9.999999747378752e-06)
    log_scale = jnp.clip(jax.random.uniform(streams_of[6], (), jnp.float32, 4.2, 4.8), 4.2, 4.8)
    bias = jnp.clip(jax.random.uniform(streams_of[7], (), jnp.float32, -16.0, -12.0), -16.0, -12.0)
    return dict(pooled=pooled, hidden=hidden, text=text, weight=weight, row_moment=row_moment, col_moment=col_moment, log_scale=log_scale, bias=bias)


EPSILON = 1e-06
DECAY_RATE = 0.8
CLIP_LEVEL = 1.0
FLOOR_VALUE = 1e-30

def reference(pooled, hidden, text, weight, row_moment, col_moment, log_scale, bias):
    batch_total = TOK_DEV * N_ROW * N_COL
    weight_half = weight.astype(jnp.bfloat16)
    projected = jnp.dot(hidden, weight_half.T, preferred_element_type=jnp.float32)
    mixed_rows = pooled.astype(jnp.float32) + projected
    length = jnp.sqrt(lax.optimization_barrier(jnp.sum(mixed_rows * mixed_rows, axis=1, keepdims=True)) + EPSILON)
    image_unit = mixed_rows / length
    images = image_unit.astype(jnp.bfloat16)
    text_float = text.astype(jnp.float32)
    text_units = (text_float / jnp.sqrt(lax.optimization_barrier(jnp.sum(text_float * text_float, axis=1, keepdims=True)) + EPSILON)).astype(jnp.bfloat16)
    logit_scale = jnp.exp(log_scale.astype(jnp.float32))
    block_rows = batch_total // N_ROW
    image_blocks = images.reshape(N_ROW, block_rows, D)
    text_ids = jnp.arange(batch_total, dtype=jnp.int32)

    def one_block(block_item):
        image_block, block_index = block_item
        image_ids = block_index * block_rows + jnp.arange(block_rows, dtype=jnp.int32)
        logits = logit_scale * jnp.dot(image_block, text_units.T, preferred_element_type=jnp.float32) + bias
        label_sign = jnp.where(image_ids[:, None] == text_ids[None, :], jnp.float32(1.0), jnp.float32(-1.0))
        loss_sum = jnp.sum(jax.nn.softplus(-label_sign * logits))
        grad_logits = (-label_sign * jax.nn.sigmoid(-label_sign * logits) / batch_total).astype(jnp.bfloat16)
        return (loss_sum, logit_scale * jnp.dot(grad_logits, text_units, preferred_element_type=jnp.float32))
    loss_sums, unit_grads = lax.map(one_block, (image_blocks, jnp.arange(N_ROW, dtype=jnp.int32)))
    loss = jnp.sum(loss_sums) / batch_total
    unit_grad = unit_grads.reshape(batch_total, D)
    mixed_grad = ((unit_grad - image_unit * lax.optimization_barrier(jnp.sum(image_unit * unit_grad, axis=1, keepdims=True))) / length).astype(jnp.bfloat16)
    gradient = jnp.dot(mixed_grad.T, hidden, preferred_element_type=jnp.float32)
    squared = gradient * gradient + FLOOR_VALUE
    new_row = DECAY_RATE * row_moment + (1.0 - DECAY_RATE) * lax.optimization_barrier(jnp.mean(squared, axis=1))
    new_col = DECAY_RATE * col_moment + (1.0 - DECAY_RATE) * lax.optimization_barrier(jnp.mean(squared, axis=0))
    second = new_row[:, None] * new_col[None, :]
    raw_update = gradient / jnp.sqrt(second)
    update_rms = jnp.sqrt(jnp.mean(raw_update * raw_update))
    update = raw_update / jnp.maximum(1.0, update_rms / CLIP_LEVEL)
    return (update, new_row, new_col, loss)
```

```python
import functools

import jax
import jax.numpy as jnp
from jax import lax
from jax.experimental import pallas as pl
from jax.experimental.pallas import tpu as pltpu
from jax.sharding import PartitionSpec as P

EPSILON = 1e-06
DECAY_RATE = 0.8
CLIP_LEVEL = 1.0
FLOOR_VALUE = 1e-30
CORES = 2
LOW = 2
MESH = pl.DeviceIdType.MESH
F32 = jnp.float32
BF16 = jnp.bfloat16


def dot_nt(a, b):
    return lax.dot_general(a, b, (((1,), (1,)), ((), ())), preferred_element_type=F32)


def kernel(
    sizes,
    hs_ref, wh_ref, pool_ref, tx_ref, rm_ref, cm_ref, ls_ref, bias_ref,
    upd_ref, nr_ref, nc_ref, loss_ref,
    hid, wg, txa, part, proj, img_s, img_r, ug_s, ug_r, mg_s, mga, gz_s, gz,
    rsb, csb, stb,
    hid_ss, hid_rs, w_ss, w_rs, tz_ss, tp_ss, t_rs, p_ss, p_rs, pair_ss, pair_rs,
    mg_ss, mg_rs, g_ss, g_rs, row_ss, row_rs, col_ss, col_rs, st_ss, st_rs,
):
    R, C, X, Z, T, Db, Dp, Fb, chunk = sizes
    L = LOW
    plane = R * L
    devices = R * C
    batch = devices * T
    r = lax.axis_index("row")
    c = lax.axis_index("col")
    z, y = c // L, c % L
    x, core = r // CORES, r % CORES
    q = r * L + y
    finish = []

    def send(src, dst, ss, rs, device, cond=None):
        def make():
            return pltpu.make_async_remote_copy(
                src_ref=src, dst_ref=dst, send_sem=ss, recv_sem=rs,
                device_id=device, device_id_type=MESH,
            )

        if cond is None:
            make().start()
            finish.append(lambda: make().wait_send())
        else:
            pl.when(cond)(lambda: make().start())
            finish.append(lambda: pl.when(cond)(lambda: make().wait_send()))

    def arrived(slot, rs):
        pltpu.make_async_copy(slot, slot, rs).wait()

    def plane_peer(o):
        other = lax.rem(q + o, plane)
        return other, other // L, other % L

    def rows(index, count):
        return pl.ds(pl.multiple_of(index * count, count), count)

    for o in range(1, plane):
        _, r2, y2 = plane_peer(o)
        send(hs_ref.at[r2], hid.at[rows(q, T)], hid_ss.at[o], hid_rs.at[q], (r2, z * L + y2))
    hid[rows(q, T)] = hs_ref[r]

    wg[rows(z, Dp)] = wh_ref[...]
    own_slot = x * C + c
    txa[:, rows(own_slot, T), :] = tx_ref[...]

    def text_place(zs):
        return x * C + zs * L + y

    for s in range(Z):
        for d, direction in enumerate((1, -1)):
            zs = z - direction * s
            nz = z + direction
            has = jnp.logical_and(zs >= 0, zs < Z)
            go = jnp.logical_and(has, jnp.logical_and(nz >= 0, nz < Z))
            place = text_place(jnp.clip(zs, 0, Z - 1))
            at = txa.at[:, rows(place, T), :]
            source = tx_ref if s == 0 else at
            if s:
                pl.when(has)(lambda: arrived(at, t_rs.at[place]))
            send(source, at, tz_ss.at[d, s], t_rs.at[place], (r, jnp.clip(nz, 0, Z - 1) * L + y), go)
            if s or d == 0:
                mine = x * L + y
                for o in range(1, X * L):
                    other = lax.rem(mine + o, X * L)
                    send(
                        source, at, tp_ss.at[d, s, o], t_rs.at[place],
                        ((other // L) * CORES + core, z * L + other % L),
                        has if s else None,
                    )
        for d, direction in enumerate((1, -1)):
            zs = z - direction * s
            nz = z + direction
            has = jnp.logical_and(zs >= 0, zs < Z)
            go = jnp.logical_and(has, jnp.logical_and(nz >= 0, nz < Z))
            block = jnp.clip(zs, 0, Z - 1)
            at = wg.at[rows(block, Dp)]
            if s:
                pl.when(has)(lambda: arrived(at, w_rs.at[block]))
            send(
                wh_ref if s == 0 else at, at, w_ss.at[d, s], w_rs.at[block],
                (r, jnp.clip(nz, 0, Z - 1) * L + y), go,
            )
    for o in range(1, plane):
        other, _, _ = plane_peer(o)
        arrived(hid.at[rows(other, T)], hid_rs.at[other])

    part[...] = dot_nt(hid[...], wg[...])
    for o in range(1, plane):
        other, r2, y2 = plane_peer(o)
        send(part.at[rows(other, T)], proj.at[r, y], p_ss.at[o], p_rs.at[q], (r2, z * L + y2))
    proj[r, y] = part[rows(q, T)]
    for o in range(1, plane):
        other, r2, y2 = plane_peer(o)
        arrived(proj.at[r2, y2], p_rs.at[other])
    mixed = []
    for h in range(L):
        total = proj[0, h]
        for k in range(1, R):
            total = total + proj[k, h]
        mixed.append(pool_ref[h].astype(F32) + total)
    square = sum(jnp.sum(m * m, axis=1, keepdims=True) for m in mixed)
    length = jnp.sqrt(square + EPSILON)
    unit = [m / length for m in mixed]
    for h in range(L):
        img_s[h] = unit[h].astype(BF16)
    partner = (x * CORES + (1 - core), c)
    send(img_s, img_r, pair_ss.at[0], pair_rs.at[0], partner)

    for o in range(1, X * L):
        other = lax.rem(x * L + y + o, X * L)
        for zs in range(Z):
            place = (other // L) * C + zs * L + other % L
            arrived(txa.at[:, rows(place, T), :], t_rs.at[place])

    scale = jnp.exp(jnp.full((1, 1), ls_ref[0], F32))
    bias = jnp.full((1, 1), bias_ref[0], F32)
    steps = X * C * T // chunk

    def pairs(images, own):
        halves = [images[h] for h in range(L)]

        def step(i, carry):
            loss, grads = carry
            cut = pl.ds(pl.multiple_of(i * chunk, chunk), chunk)
            texts = [txa[h, cut, :] for h in range(L)]
            logits = scale * sum(dot_nt(halves[h], texts[h]) for h in range(L)) + bias
            if own:
                row_id = lax.broadcasted_iota(jnp.int32, logits.shape, 0) + own_slot * T
                col_id = lax.broadcasted_iota(jnp.int32, logits.shape, 1) + i * chunk
                sign = jnp.where(row_id == col_id, F32(1.0), F32(-1.0))
            else:
                sign = F32(-1.0)
            u = -sign * logits
            e = jnp.exp(-jnp.abs(u))
            loss = loss + jnp.sum(jnp.maximum(u, 0.0) + jnp.log1p(e), axis=1, keepdims=True)
            sig = jnp.where(u >= 0, F32(1.0), e) / (1.0 + e)
            pg = (-sign * sig / batch).astype(BF16)
            grads = tuple(
                grads[h] + jnp.dot(pg, texts[h], preferred_element_type=F32) for h in range(L)
            )
            return loss, grads

        zero = (jnp.zeros((T, 1), F32), tuple(jnp.zeros((T, Z * Dp), F32) for _ in range(L)))
        if steps == 1:
            return step(0, zero)
        return lax.fori_loop(0, steps, step, zero)

    arrived(img_r, pair_rs.at[0])
    loss_b, grads_b = pairs(img_r, False)
    for h in range(L):
        ug_s[h] = scale * grads_b[h]
    send(ug_s, ug_r, pair_ss.at[1], pair_rs.at[1], partner)
    loss_a, grads_a = pairs(img_s, True)
    arrived(ug_r, pair_rs.at[1])
    ug = [scale * grads_a[h] + ug_r[h] for h in range(L)]
    inner = sum(jnp.sum(unit[h] * ug[h], axis=1, keepdims=True) for h in range(L))
    for h in range(L):
        mg_s[h] = ((ug[h] - unit[h] * inner) / length).astype(BF16)
    for o in range(1, plane):
        _, r2, y2 = plane_peer(o)
        send(mg_s.at[y2], mga.at[rows(q, T)], mg_ss.at[o], mg_rs.at[q], (r2, z * L + y2))
    mga[rows(q, T)] = mg_s[y]
    for o in range(1, plane):
        other, _, _ = plane_peer(o)
        arrived(mga.at[rows(other, T)], mg_rs.at[other])

    turned = mga[...].T
    for zs in range(Z):
        gz_s[zs] = jnp.dot(
            turned[zs * Dp:(zs + 1) * Dp], hid[...], preferred_element_type=F32
        ).astype(BF16)
    for o in range(1, Z):
        z2 = lax.rem(z + o, Z)
        send(gz_s.at[z2], gz.at[z], g_ss.at[o], g_rs.at[z], (r, z2 * L + y))
    upd_ref[...] = own_block(turned, hid, z, Z, Dp, Db)
    for o in range(1, Z):
        z2 = lax.rem(z + o, Z)
        arrived(gz.at[z2], g_rs.at[z2])
        upd_ref[...] += gz[z2][:Db].astype(F32)
    g = upd_ref[...]

    sq = g * g + FLOOR_VALUE
    rsb[r] = jnp.sum(sq, axis=1, keepdims=True)
    csb[c] = jnp.sum(sq, axis=0, keepdims=True)
    for o in range(1, C):
        c2 = lax.rem(c + o, C)
        send(csb.at[c], csb.at[c], col_ss.at[o], col_rs.at[c], (r, c2))
    for o in range(1, R):
        r2 = lax.rem(r + o, R)
        send(rsb.at[r], rsb.at[r], row_ss.at[o], row_rs.at[r], (r2, c))
    for o in range(1, R):
        r2 = lax.rem(r + o, R)
        arrived(rsb.at[r2], row_rs.at[r2])
    for o in range(1, C):
        c2 = lax.rem(c + o, C)
        arrived(csb.at[c2], col_rs.at[c2])
    row_sum = sum(rsb[k] for k in range(R))
    col_sum = sum(csb[k] for k in range(C))
    new_row = DECAY_RATE * rm_ref[...] + (1.0 - DECAY_RATE) * row_sum / (R * Fb)
    new_col = DECAY_RATE * cm_ref[...] + (1.0 - DECAY_RATE) * col_sum / (C * Db)
    nr_ref[...] = new_row
    nc_ref[...] = new_col
    raw = g / jnp.sqrt(new_row * new_col)
    upd_ref[...] = raw
    local = jnp.sum(jnp.sum(raw * raw, axis=1, keepdims=True), axis=0, keepdims=True)
    loss_local = jnp.sum(loss_a + loss_b, axis=0, keepdims=True)
    lane = lax.broadcasted_iota(jnp.int32, (1, 128), 1)
    me = r * C + c
    stb[me] = jnp.where(lane == 0, local, loss_local)

    def tell(o, wait):
        other = lax.rem(me + o, devices)
        copy = pltpu.make_async_remote_copy(
            src_ref=stb.at[me], dst_ref=stb.at[me], send_sem=st_ss.at[o], recv_sem=st_rs.at[me],
            device_id=(other // C, other % C), device_id_type=MESH,
        )
        if wait:
            copy.wait_send()
            arrived(stb.at[other], st_rs.at[other])
        else:
            copy.start()

    def tell_start(o, _):
        tell(o, False)
        return _

    def tell_wait(o, _):
        tell(o, True)
        return _

    lax.fori_loop(1, devices, tell_start, 0)
    lax.fori_loop(1, devices, tell_wait, 0)
    totals = jnp.sum(stb[...], axis=0)
    rms = jnp.sqrt(totals[:, 0:1] / (C * Db * R * Fb))
    upd_ref[...] = upd_ref[...] / jnp.maximum(1.0, rms / CLIP_LEVEL)
    loss_ref[...] = totals / batch
    for wait in finish:
        wait()


def own_block(turned, hid, z, Z, Dp, Db):
    picked = turned[0:Dp]
    for zs in range(1, Z):
        picked = jnp.where(z == zs, turned[zs * Dp:(zs + 1) * Dp], picked)
    return jnp.dot(picked, hid[...], preferred_element_type=F32)[:Db]


def per_device(pooled, hidden, text, weight, row_moment, col_moment, log_scale, bias):
    R, C = lax.axis_size("row"), lax.axis_size("col")
    L, X, Z = LOW, R // CORES, C // LOW
    T, D = pooled.shape
    Db, Fb = weight.shape
    Dp = -(-Db // 16) * 16
    F2 = Z * Dp
    plane = R * L
    texts = X * C * T
    chunk = min(texts, 512)

    def by_half(a):
        a = a.reshape(T, Z, L, Db).transpose(2, 0, 1, 3)
        if Dp != Db:
            a = jnp.pad(a, ((0, 0), (0, 0), (0, 0), (0, Dp - Db)))
        return a.reshape(L, T, F2)

    hs = hidden.reshape(T, R, Fb).transpose(1, 0, 2)
    wh = weight.astype(BF16)
    if Dp != Db:
        wh = jnp.pad(wh, ((0, Dp - Db), (0, 0)))
    tf = text.astype(F32)
    tn = (tf / jnp.sqrt(jnp.sum(tf * tf, axis=1, keepdims=True) + EPSILON)).astype(BF16)
    sizes = (R, C, X, Z, T, Db, Dp, Fb, chunk)
    vmem = pl.BlockSpec(memory_space=pltpu.VMEM)
    smem = pl.BlockSpec(memory_space=pltpu.SMEM)
    dma = lambda *s: pltpu.SemaphoreType.DMA(s)
    upd, nr, nc, loss = pl.pallas_call(
        functools.partial(kernel, sizes),
        out_shape=(
            jax.ShapeDtypeStruct((Db, Fb), F32),
            jax.ShapeDtypeStruct((Db, 1), F32),
            jax.ShapeDtypeStruct((1, Fb), F32),
            jax.ShapeDtypeStruct((1, 128), F32),
        ),
        in_specs=[vmem] * 6 + [smem] * 2,
        out_specs=(vmem,) * 4,
        scratch_shapes=[
            pltpu.VMEM((plane * T, Fb), BF16),
            pltpu.VMEM((F2, Fb), BF16),
            pltpu.VMEM((L, texts, F2), BF16),
            pltpu.VMEM((plane * T, F2), F32),
            pltpu.VMEM((R, L, T, F2), F32),
            pltpu.VMEM((L, T, F2), BF16),
            pltpu.VMEM((L, T, F2), BF16),
            pltpu.VMEM((L, T, F2), F32),
            pltpu.VMEM((L, T, F2), F32),
            pltpu.VMEM((L, T, F2), BF16),
            pltpu.VMEM((plane * T, F2), BF16),
            pltpu.VMEM((Z, Dp, Fb), BF16),
            pltpu.VMEM((Z, Dp, Fb), BF16),
            pltpu.VMEM((R, Db, 1), F32),
            pltpu.VMEM((C, 1, Fb), F32),
            pltpu.VMEM((R * C, 1, 128), F32),
            dma(plane), dma(plane), dma(2, Z), dma(Z), dma(2, Z), dma(2, Z, X * L), dma(X * C),
            dma(plane), dma(plane), dma(2), dma(2), dma(plane), dma(plane), dma(Z), dma(Z),
            dma(R), dma(R), dma(C), dma(C), dma(R * C), dma(R * C),
        ],
        compiler_params=pltpu.CompilerParams(
            has_side_effects=True, vmem_limit_bytes=60 * 1024 * 1024
        ),
    )(
        hs, wh, by_half(pooled), by_half(tn), row_moment[:, None], col_moment[None, :],
        log_scale[None], bias[None],
    )
    return upd, nr[:, 0], nc[0], loss[0, 1]


def solution(mesh):
    return jax.shard_map(
        per_device,
        mesh=mesh,
        in_specs=(
            P(("row", "col"), None),
            P(("row", "col"), None),
            P(("row", "col"), None),
            P("col", "row"),
            P("col"),
            P("row"),
            P(),
            P(),
        ),
        out_specs=(P("col", "row"), P("col"), P("row"), P()),
        check_vma=False,
    )
```

```python
import functools

import jax
import jax.numpy as jnp
from jax import lax
from jax.experimental import pallas as pl
from jax.experimental.pallas import tpu as pltpu
from jax.sharding import PartitionSpec as P

EPSILON = 1e-06
DECAY_RATE = 0.8
CLIP_LEVEL = 1.0
FLOOR_VALUE = 1e-30
CORES = 2
LOW = 2
MESH = pl.DeviceIdType.MESH
F32 = jnp.float32
BF16 = jnp.bfloat16


def dot_nt(a, b):
    return lax.dot_general(a, b, (((1,), (1,)), ((), ())), preferred_element_type=F32)


def kernel(
    sizes,
    hs_ref, wh_ref, pool_ref, tx_ref, rm_ref, cm_ref, ls_ref, bias_ref,
    upd_ref, nr_ref, nc_ref, loss_ref,
    hid, wg, txa, part, pre, summed, proj, img_s, img_r, ug_s, ug_r, mg_s, mga, gp, gz_s, gz,
    rsb, csb, stb,
    hid_ss, hid_rs, w_ss, w_rs, tz_ss, tp_ss, t_rs, td_ss, td_rs, pp_ss, pp_rs, p_ss, p_rs, pair_ss, pair_rs,
    mg_ss, mg_rs, g_ss, g_rs, row_ss, row_rs, col_ss, col_rs, st_ss, st_rs,
):
    R, C, X, Z, T, Db, Dp, Fb, chunk = sizes
    L = LOW
    plane = R * L
    devices = R * C
    batch = devices * T
    r = lax.axis_index("row")
    c = lax.axis_index("col")
    z, y = c // L, c % L
    x, core = r // CORES, r % CORES
    q = r * L + y
    finish = []

    def send(src, dst, ss, rs, device, cond=None):
        def make():
            return pltpu.make_async_remote_copy(
                src_ref=src, dst_ref=dst, send_sem=ss, recv_sem=rs,
                device_id=device, device_id_type=MESH,
            )

        if cond is None:
            make().start()
            finish.append(lambda: make().wait_send())
        else:
            pl.when(cond)(lambda: make().start())
            finish.append(lambda: pl.when(cond)(lambda: make().wait_send()))

    def arrived(slot, rs):
        pltpu.make_async_copy(slot, slot, rs).wait()

    def plane_peer(o):
        other = lax.rem(q + o, plane)
        return other, other // L, other % L

    def rows(index, count):
        return pl.ds(pl.multiple_of(index * count, count), count)

    for o in range(1, plane):
        _, r2, y2 = plane_peer(o)
        send(hs_ref.at[r2], hid.at[rows(q, T)], hid_ss.at[o], hid_rs.at[q], (r2, z * L + y2))
    hid[rows(q, T)] = hs_ref[r]

    wg[rows(z, Dp)] = wh_ref[...]
    own_slot = x * C + c
    txa[:, rows(own_slot, T), :] = tx_ref[...]

    def text_place(zs):
        return x * C + zs * L + y

    def neighbours():
        along_x = [(lax.rem(x + o, X), y) for o in range(1, X)]
        return along_x + [(x, lax.rem(y + o, L)) for o in range(1, L)]

    def relay(s):
        for d, direction in enumerate((1, -1)):
            if s == 0 and d:
                continue
            zs = z - direction * s
            has = jnp.logical_and(zs >= 0, zs < Z)
            block = jnp.clip(zs, 0, Z - 1)
            for n, (x2, y2) in enumerate(neighbours()):
                place = x2 * C + block * L + y2
                at = txa.at[:, rows(place, T), :]
                if s:
                    pl.when(has)(lambda: arrived(at, t_rs.at[place]))
                else:
                    arrived(at, t_rs.at[place])
                h = 0 if n < X - 1 else 1
                half = txa.at[h, rows(place, T), :]
                onward = neighbours()[X - 1:] if h == 0 else neighbours()[:X - 1]
                for m, (x3, y3) in enumerate(onward):
                    send(
                        half, half, td_ss.at[d, s, n, m], td_rs.at[place, h],
                        (x3 * CORES + core, z * L + y3), has if s else None,
                    )

    for s in range(Z):
        for d, direction in enumerate((1, -1)):
            zs = z - direction * s
            nz = z + direction
            has = jnp.logical_and(zs >= 0, zs < Z)
            go = jnp.logical_and(has, jnp.logical_and(nz >= 0, nz < Z))
            place = text_place(jnp.clip(zs, 0, Z - 1))
            at = txa.at[:, rows(place, T), :]
            source = tx_ref if s == 0 else at
            if s:
                pl.when(has)(lambda: arrived(at, t_rs.at[place]))
            send(source, at, tz_ss.at[d, s], t_rs.at[place], (r, jnp.clip(nz, 0, Z - 1) * L + y), go)
            if s or d == 0:
                for n, (x2, y2) in enumerate(neighbours()):
                    send(
                        source, at, tp_ss.at[d, s, n], t_rs.at[place],
                        (x2 * CORES + core, z * L + y2), has if s else None,
                    )
        for d, direction in enumerate((1, -1)):
            zs = z - direction * s
            nz = z + direction
            has = jnp.logical_and(zs >= 0, zs < Z)
            go = jnp.logical_and(has, jnp.logical_and(nz >= 0, nz < Z))
            block = jnp.clip(zs, 0, Z - 1)
            at = wg.at[rows(block, Dp)]
            if s:
                pl.when(has)(lambda: arrived(at, w_rs.at[block]))
            send(
                wh_ref if s == 0 else at, at, w_ss.at[d, s], w_rs.at[block],
                (r, jnp.clip(nz, 0, Z - 1) * L + y), go,
            )
        if s:
            relay(s - 1)
    for o in range(1, plane):
        other, _, _ = plane_peer(o)
        arrived(hid.at[rows(other, T)], hid_rs.at[other])

    part[...] = dot_nt(hid[...], wg[...])
    partner = (x * CORES + (1 - core), c)
    for o in range(1, X + 1):
        x2 = lax.rem(x + o, X)
        send(
            part.at[rows(x2 * CORES + 1 - core, L * T)], pre.at[x2],
            pp_ss.at[o], pp_rs.at[x2], partner,
        )
    relay(Z - 1)
    for o in range(1, X + 1):
        x2 = lax.rem(x + o, X)
        arrived(pre.at[x2], pp_rs.at[x2])
        summed[x2] = part[rows(x2 * CORES + core, L * T)] + pre[x2]
        for k in range(L):
            y2 = lax.rem(y + 1 + k, L)
            if o == X and k == L - 1:
                proj[x, y] = summed[x, rows(y, T)]
            else:
                send(
                    summed.at[x2, rows(y2, T)], proj.at[x, y], p_ss.at[o * L + k],
                    p_rs.at[x * L + y], (x2 * CORES + core, z * L + y2),
                )
    for o in range(1, X * L):
        other = lax.rem(x * L + y + o, X * L)
        arrived(proj.at[other // L, other % L], p_rs.at[other])
    mixed = []
    for h in range(L):
        total = proj[0, h]
        for k in range(1, X):
            total = total + proj[k, h]
        mixed.append(pool_ref[h].astype(F32) + total)
    square = sum(jnp.sum(m * m, axis=1, keepdims=True) for m in mixed)
    length = jnp.sqrt(square + EPSILON)
    unit = [m / length for m in mixed]
    for h in range(L):
        img_s[h] = unit[h].astype(BF16)
    send(img_s, img_r, pair_ss.at[0], pair_rs.at[0], partner)

    for ox in range(1, X):
        for oy in range(1, L):
            for zs in range(Z):
                place = lax.rem(x + ox, X) * C + zs * L + lax.rem(y + oy, L)
                for h in range(L):
                    arrived(txa.at[h, rows(place, T), :], td_rs.at[place, h])

    scale = jnp.exp(jnp.full((1, 1), ls_ref[0], F32))
    bias = jnp.full((1, 1), bias_ref[0], F32)
    steps = X * C * T // chunk

    def pairs(images, own):
        halves = [images[h] for h in range(L)]

        def step(i, carry):
            loss, grads = carry
            cut = pl.ds(pl.multiple_of(i * chunk, chunk), chunk)
            texts = [txa[h, cut, :] for h in range(L)]
            logits = scale * sum(dot_nt(halves[h], texts[h]) for h in range(L)) + bias
            if own:
                row_id = lax.broadcasted_iota(jnp.int32, logits.shape, 0) + own_slot * T
                col_id = lax.broadcasted_iota(jnp.int32, logits.shape, 1) + i * chunk
                sign = jnp.where(row_id == col_id, F32(1.0), F32(-1.0))
            else:
                sign = F32(-1.0)
            u = -sign * logits
            e = jnp.exp(-jnp.abs(u))
            loss = loss + jnp.sum(jnp.maximum(u, 0.0) + jnp.log1p(e), axis=1, keepdims=True)
            sig = jnp.where(u >= 0, F32(1.0), e) / (1.0 + e)
            pg = (-sign * sig / batch).astype(BF16)
            grads = tuple(
                grads[h] + jnp.dot(pg, texts[h], preferred_element_type=F32) for h in range(L)
            )
            return loss, grads

        zero = (jnp.zeros((T, 1), F32), tuple(jnp.zeros((T, Z * Dp), F32) for _ in range(L)))
        if steps == 1:
            return step(0, zero)
        return lax.fori_loop(0, steps, step, zero)

    arrived(img_r, pair_rs.at[0])
    loss_b, grads_b = pairs(img_r, False)
    for h in range(L):
        ug_s[h] = scale * grads_b[h]
    send(ug_s, ug_r, pair_ss.at[1], pair_rs.at[1], partner)
    loss_a, grads_a = pairs(img_s, True)
    arrived(ug_r, pair_rs.at[1])
    ug = [scale * grads_a[h] + ug_r[h] for h in range(L)]
    inner = sum(jnp.sum(unit[h] * ug[h], axis=1, keepdims=True) for h in range(L))
    for h in range(L):
        mg_s[h] = ((ug[h] - unit[h] * inner) / length).astype(BF16)
    for o in range(1, X * L):
        other = lax.rem(x * L + y + o, X * L)
        send(
            mg_s.at[other % L], mga.at[rows(q, T)], mg_ss.at[o], mg_rs.at[q],
            ((other // L) * CORES + core, z * L + other % L),
        )
    send(mg_s.at[y], mga.at[rows(q, T)], mg_ss.at[0], mg_rs.at[q], partner)
    mga[rows(q, T)] = mg_s[y]
    for o in range(1, X * L):
        other = lax.rem(x * L + y + o, X * L)
        source = ((other // L) * CORES + core) * L + other % L
        at = mga.at[rows(source, T)]
        arrived(at, mg_rs.at[source])
        send(at, at, mg_ss.at[X * L + o], mg_rs.at[source], partner)
    for o in range(X * L):
        other = lax.rem(x * L + y + o, X * L)
        source = ((other // L) * CORES + 1 - core) * L + other % L
        arrived(mga.at[rows(source, T)], mg_rs.at[source])

    turned = mga[...].T

    def own_part(zd):
        gp[zd] = jnp.dot(turned[zd * Dp:(zd + 1) * Dp], hid[...], preferred_element_type=F32)

    def pass_on(zd, d, direction):
        first = z == (0 if d == 0 else Z - 1)
        before = z < zd if d == 0 else z > zd

        def add():
            arrived(gz.at[d, zd], g_rs.at[d, zd])
            gz_s[zd] = (gp[zd] + gz[d, zd].astype(F32)).astype(BF16)

        def start():
            gz_s[zd] = gp[zd].astype(BF16)

        pl.when(jnp.logical_and(before, first))(start)
        pl.when(jnp.logical_and(before, jnp.logical_not(first)))(add)
        send(
            gz_s.at[zd], gz.at[d, zd], g_ss.at[d, zd], g_rs.at[d, zd],
            (r, jnp.clip(z + direction, 0, Z - 1) * L + y), before,
        )

    for k in range(Z):
        up, down = Z - 1 - k, k
        if k < (Z + 1) // 2:
            own_part(up)
            if down != up:
                own_part(down)
        pass_on(up, 0, 1)
        pass_on(down, 1, -1)
    upd_ref[...] = gp[z][:Db]
    for d in range(2):
        def take():
            arrived(gz.at[d, z], g_rs.at[d, z])
            upd_ref[...] += gz[d, z][:Db].astype(F32)

        pl.when(z > 0 if d == 0 else z < Z - 1)(take)
    g = upd_ref[...]

    sq = g * g + FLOOR_VALUE
    rsb[r] = jnp.sum(sq, axis=1, keepdims=True)
    csb[c] = jnp.sum(sq, axis=0, keepdims=True)
    for o in range(1, C):
        c2 = lax.rem(c + o, C)
        send(csb.at[c], csb.at[c], col_ss.at[o], col_rs.at[c], (r, c2))
    for o in range(1, R):
        r2 = lax.rem(r + o, R)
        send(rsb.at[r], rsb.at[r], row_ss.at[o], row_rs.at[r], (r2, c))
    for o in range(1, R):
        r2 = lax.rem(r + o, R)
        arrived(rsb.at[r2], row_rs.at[r2])
    for o in range(1, C):
        c2 = lax.rem(c + o, C)
        arrived(csb.at[c2], col_rs.at[c2])
    row_sum = sum(rsb[k] for k in range(R))
    col_sum = sum(csb[k] for k in range(C))
    new_row = DECAY_RATE * rm_ref[...] + (1.0 - DECAY_RATE) * row_sum / (R * Fb)
    new_col = DECAY_RATE * cm_ref[...] + (1.0 - DECAY_RATE) * col_sum / (C * Db)
    nr_ref[...] = new_row
    nc_ref[...] = new_col
    raw = g / jnp.sqrt(new_row * new_col)
    upd_ref[...] = raw
    local = jnp.sum(jnp.sum(raw * raw, axis=1, keepdims=True), axis=0, keepdims=True)
    loss_local = jnp.sum(loss_a + loss_b, axis=0, keepdims=True)
    lane = lax.broadcasted_iota(jnp.int32, (1, 128), 1)
    me = r * C + c
    stb[me] = jnp.where(lane == 0, local, loss_local)

    def tell(o, wait):
        other = lax.rem(me + o, devices)
        copy = pltpu.make_async_remote_copy(
            src_ref=stb.at[me], dst_ref=stb.at[me], send_sem=st_ss.at[o], recv_sem=st_rs.at[me],
            device_id=(other // C, other % C), device_id_type=MESH,
        )
        if wait:
            copy.wait_send()
            arrived(stb.at[other], st_rs.at[other])
        else:
            copy.start()

    def tell_start(o, _):
        tell(o, False)
        return _

    def tell_wait(o, _):
        tell(o, True)
        return _

    lax.fori_loop(1, devices, tell_start, 0)
    lax.fori_loop(1, devices, tell_wait, 0)
    totals = jnp.sum(stb[...], axis=0)
    rms = jnp.sqrt(totals[:, 0:1] / (C * Db * R * Fb))
    upd_ref[...] = upd_ref[...] / jnp.maximum(1.0, rms / CLIP_LEVEL)
    loss_ref[...] = totals / batch
    for wait in finish:
        wait()


def per_device(pooled, hidden, text, weight, row_moment, col_moment, log_scale, bias):
    R, C = lax.axis_size("row"), lax.axis_size("col")
    L, X, Z = LOW, R // CORES, C // LOW
    T, D = pooled.shape
    Db, Fb = weight.shape
    Dp = -(-Db // 16) * 16
    F2 = Z * Dp
    plane = R * L
    texts = X * C * T
    chunk = min(texts, 512)

    def by_half(a):
        a = a.reshape(T, Z, L, Db).transpose(2, 0, 1, 3)
        if Dp != Db:
            a = jnp.pad(a, ((0, 0), (0, 0), (0, 0), (0, Dp - Db)))
        return a.reshape(L, T, F2)

    hs = hidden.reshape(T, R, Fb).transpose(1, 0, 2)
    wh = weight.astype(BF16)
    if Dp != Db:
        wh = jnp.pad(wh, ((0, Dp - Db), (0, 0)))
    tf = text.astype(F32)
    tn = (tf / jnp.sqrt(jnp.sum(tf * tf, axis=1, keepdims=True) + EPSILON)).astype(BF16)
    sizes = (R, C, X, Z, T, Db, Dp, Fb, chunk)
    vmem = pl.BlockSpec(memory_space=pltpu.VMEM)
    smem = pl.BlockSpec(memory_space=pltpu.SMEM)
    dma = lambda *s: pltpu.SemaphoreType.DMA(s)
    upd, nr, nc, loss = pl.pallas_call(
        functools.partial(kernel, sizes),
        out_shape=(
            jax.ShapeDtypeStruct((Db, Fb), F32),
            jax.ShapeDtypeStruct((Db, 1), F32),
            jax.ShapeDtypeStruct((1, Fb), F32),
            jax.ShapeDtypeStruct((1, 128), F32),
        ),
        in_specs=[vmem] * 6 + [smem] * 2,
        out_specs=(vmem,) * 4,
        scratch_shapes=[
            pltpu.VMEM((plane * T, Fb), BF16),
            pltpu.VMEM((F2, Fb), BF16),
            pltpu.VMEM((L, texts, F2), BF16),
            pltpu.VMEM((plane * T, F2), F32),
            pltpu.VMEM((X, L * T, F2), F32),
            pltpu.VMEM((X, L * T, F2), F32),
            pltpu.VMEM((X, L, T, F2), F32),
            pltpu.VMEM((L, T, F2), BF16),
            pltpu.VMEM((L, T, F2), BF16),
            pltpu.VMEM((L, T, F2), F32),
            pltpu.VMEM((L, T, F2), F32),
            pltpu.VMEM((L, T, F2), BF16),
            pltpu.VMEM((plane * T, F2), BF16),
            pltpu.VMEM((Z, Dp, Fb), F32),
            pltpu.VMEM((Z, Dp, Fb), BF16),
            pltpu.VMEM((2, Z, Dp, Fb), BF16),
            pltpu.VMEM((R, Db, 1), F32),
            pltpu.VMEM((C, 1, Fb), F32),
            pltpu.VMEM((R * C, 1, 128), F32),
            dma(plane), dma(plane), dma(2, Z), dma(Z), dma(2, Z), dma(2, Z, X + L), dma(X * C),
            dma(2, Z, X + L, X + L), dma(X * C, L), dma(X + 1), dma(X), dma(X * L + L), dma(X * L),
            dma(2), dma(2), dma(plane), dma(plane), dma(2, Z), dma(2, Z),
            dma(R), dma(R), dma(C), dma(C), dma(R * C), dma(R * C),
        ],
        compiler_params=pltpu.CompilerParams(
            has_side_effects=True, vmem_limit_bytes=60 * 1024 * 1024
        ),
    )(
        hs, wh, by_half(pooled), by_half(tn), row_moment[:, None], col_moment[None, :],
        log_scale[None], bias[None],
    )
    return upd, nr[:, 0], nc[0], loss[0, 1]


def solution(mesh):
    return jax.shard_map(
        per_device,
        mesh=mesh,
        in_specs=(
            P(("row", "col"), None),
            P(("row", "col"), None),
            P(("row", "col"), None),
            P("col", "row"),
            P("col"),
            P("row"),
            P(),
            P(),
        ),
        out_specs=(P("col", "row"), P("col"), P("row"), P()),
        check_vma=False,
    )
```

```python
import functools

import jax
import jax.numpy as jnp
from jax import lax
from jax.experimental import pallas as pl
from jax.experimental.pallas import tpu as pltpu
from jax.sharding import PartitionSpec as P

EPSILON = 1e-06
DECAY_RATE = 0.8
CLIP_LEVEL = 1.0
FLOOR_VALUE = 1e-30
CORES = 2
LOW = 2
MESH = pl.DeviceIdType.MESH
F32 = jnp.float32
BF16 = jnp.bfloat16


def dot_nt(a, b):
    return lax.dot_general(a, b, (((1,), (1,)), ((), ())), preferred_element_type=F32)


def kernel(
    sizes,
    hs_ref, wh_ref, pool_ref, tx_ref, rm_ref, cm_ref, ls_ref, bias_ref,
    upd_ref, nr_ref, nc_ref, loss_ref,
    hid, wg, txa, part, pre, summed, proj, img_s, img_r, ug_s, ug_r, mg_s, mga, gp, gz_s, gz,
    rsb, csb, stb,
    hid_ss, hid_rs, w_ss, w_rs, tz_ss, tp_ss, t_rs, td_ss, td_rs, pp_ss, pp_rs, p_ss, p_rs, pair_ss, pair_rs,
    mg_ss, mg_rs, g_ss, g_rs, row_ss, row_rs, col_ss, col_rs, st_ss, st_rs,
):
    R, C, X, Z, T, Db, Dp, Fb, chunk = sizes
    L = LOW
    plane = R * L
    devices = R * C
    batch = devices * T
    r = lax.axis_index("row")
    c = lax.axis_index("col")
    z, y = c // L, c % L
    x, core = r // CORES, r % CORES
    q = r * L + y
    finish = []

    def send(src, dst, ss, rs, device, cond=None):
        def make():
            return pltpu.make_async_remote_copy(
                src_ref=src, dst_ref=dst, send_sem=ss, recv_sem=rs,
                device_id=device, device_id_type=MESH,
            )

        if cond is None:
            make().start()
            finish.append(lambda: make().wait_send())
        else:
            pl.when(cond)(lambda: make().start())
            finish.append(lambda: pl.when(cond)(lambda: make().wait_send()))

    def arrived(slot, rs):
        pltpu.make_async_copy(slot, slot, rs).wait()

    def plane_peer(o):
        other = lax.rem(q + o, plane)
        return other, other // L, other % L

    def rows(index, count):
        return pl.ds(pl.multiple_of(index * count, count), count)

    for o in range(1, plane):
        _, r2, y2 = plane_peer(o)
        send(hs_ref.at[r2], hid.at[rows(q, T)], hid_ss.at[o], hid_rs.at[q], (r2, z * L + y2))
    hid[rows(q, T)] = hs_ref[r]

    wg[rows(z, Dp)] = wh_ref[...]
    own_slot = x * C + c
    txa[:, rows(own_slot, T), :] = tx_ref[...]

    def text_place(zs):
        return x * C + zs * L + y

    def neighbours():
        along_x = [(lax.rem(x + o, X), y) for o in range(1, X)]
        return along_x + [(x, lax.rem(y + o, L)) for o in range(1, L)]

    def relay(s):
        for d, direction in enumerate((1, -1)):
            if s == 0 and d:
                continue
            zs = z - direction * s
            has = jnp.logical_and(zs >= 0, zs < Z)
            block = jnp.clip(zs, 0, Z - 1)
            for n, (x2, y2) in enumerate(neighbours()):
                place = x2 * C + block * L + y2
                at = txa.at[:, rows(place, T), :]
                if s:
                    pl.when(has)(lambda: arrived(at, t_rs.at[place]))
                else:
                    arrived(at, t_rs.at[place])
                h = 0 if n < X - 1 else 1
                half = txa.at[h, rows(place, T), :]
                onward = neighbours()[X - 1:] if h == 0 else neighbours()[:X - 1]
                for m, (x3, y3) in enumerate(onward):
                    send(
                        half, half, td_ss.at[d, s, n, m], td_rs.at[place, h],
                        (x3 * CORES + core, z * L + y3), has if s else None,
                    )

    for s in range(Z):
        for d, direction in enumerate((1, -1)):
            zs = z - direction * s
            nz = z + direction
            has = jnp.logical_and(zs >= 0, zs < Z)
            go = jnp.logical_and(has, jnp.logical_and(nz >= 0, nz < Z))
            place = text_place(jnp.clip(zs, 0, Z - 1))
            at = txa.at[:, rows(place, T), :]
            source = tx_ref if s == 0 else at
            if s:
                pl.when(has)(lambda: arrived(at, t_rs.at[place]))
            send(source, at, tz_ss.at[d, s], t_rs.at[place], (r, jnp.clip(nz, 0, Z - 1) * L + y), go)
            if s or d == 0:
                for n, (x2, y2) in enumerate(neighbours()):
                    send(
                        source, at, tp_ss.at[d, s, n], t_rs.at[place],
                        (x2 * CORES + core, z * L + y2), has if s else None,
                    )
        for d, direction in enumerate((1, -1)):
            zs = z - direction * s
            nz = z + direction
            has = jnp.logical_and(zs >= 0, zs < Z)
            go = jnp.logical_and(has, jnp.logical_and(nz >= 0, nz < Z))
            block = jnp.clip(zs, 0, Z - 1)
            at = wg.at[rows(block, Dp)]
            if s:
                pl.when(has)(lambda: arrived(at, w_rs.at[block]))
            send(
                wh_ref if s == 0 else at, at, w_ss.at[d, s], w_rs.at[block],
                (r, jnp.clip(nz, 0, Z - 1) * L + y), go,
            )
        if s:
            relay(s - 1)
    for o in range(1, plane):
        other, _, _ = plane_peer(o)
        arrived(hid.at[rows(other, T)], hid_rs.at[other])

    part[...] = dot_nt(hid[...], wg[...])
    partner = (x * CORES + (1 - core), c)
    for o in range(1, X + 1):
        x2 = lax.rem(x + o, X)
        send(
            part.at[rows(x2 * CORES + 1 - core, L * T)], pre.at[x2],
            pp_ss.at[o], pp_rs.at[x2], partner,
        )
    relay(Z - 1)
    for o in range(1, X + 1):
        x2 = lax.rem(x + o, X)
        arrived(pre.at[x2], pp_rs.at[x2])
        summed[x2] = part[rows(x2 * CORES + core, L * T)] + pre[x2]
        for k in range(L):
            y2 = lax.rem(y + 1 + k, L)
            if o == X and k == L - 1:
                proj[x, y] = summed[x, rows(y, T)]
            else:
                send(
                    summed.at[x2, rows(y2, T)], proj.at[x, y], p_ss.at[o * L + k],
                    p_rs.at[x * L + y], (x2 * CORES + core, z * L + y2),
                )
    for o in range(1, X * L):
        other = lax.rem(x * L + y + o, X * L)
        arrived(proj.at[other // L, other % L], p_rs.at[other])
    mixed = []
    for h in range(L):
        total = proj[0, h]
        for k in range(1, X):
            total = total + proj[k, h]
        mixed.append(pool_ref[h].astype(F32) + total)
    square = sum(jnp.sum(m * m, axis=1, keepdims=True) for m in mixed)
    length = jnp.sqrt(square + EPSILON)
    unit = [m / length for m in mixed]
    for h in range(L):
        img_s[h] = unit[h].astype(BF16)
    send(img_s, img_r, pair_ss.at[0], pair_rs.at[0], partner)

    for ox in range(1, X):
        for oy in range(1, L):
            for zs in range(Z):
                place = lax.rem(x + ox, X) * C + zs * L + lax.rem(y + oy, L)
                for h in range(L):
                    arrived(txa.at[h, rows(place, T), :], td_rs.at[place, h])

    scale = jnp.exp(jnp.full((1, 1), ls_ref[0], F32))
    bias = jnp.full((1, 1), bias_ref[0], F32)
    steps = X * C * T // chunk

    def pairs():
        halves = [jnp.concatenate([img_s[h], img_r[h]], axis=0) for h in range(L)]

        def step(i, carry):
            loss, grads = carry
            cut = pl.ds(pl.multiple_of(i * chunk, chunk), chunk)
            texts = [txa[h, cut, :] for h in range(L)]
            logits = scale * sum(dot_nt(halves[h], texts[h]) for h in range(L)) + bias
            row_id = lax.broadcasted_iota(jnp.int32, logits.shape, 0)
            col_id = lax.broadcasted_iota(jnp.int32, logits.shape, 1) + (i * chunk - own_slot * T)
            match = jnp.logical_and(row_id == col_id, row_id < T)
            sign = jnp.where(match, F32(1.0), F32(-1.0))
            u = -sign * logits
            e = jnp.exp(-jnp.abs(u))
            loss = loss + jnp.sum(jnp.maximum(u, 0.0) + jnp.log1p(e), axis=1, keepdims=True)
            sig = jnp.where(u >= 0, F32(1.0), e) / (1.0 + e)
            pg = (-sign * sig / batch).astype(BF16)
            grads = tuple(
                grads[h] + jnp.dot(pg, texts[h], preferred_element_type=F32) for h in range(L)
            )
            return loss, grads

        zero = (
            jnp.zeros((2 * T, 1), F32), tuple(jnp.zeros((2 * T, Z * Dp), F32) for _ in range(L))
        )
        if steps == 1:
            return step(0, zero)
        return lax.fori_loop(0, steps, step, zero)

    arrived(img_r, pair_rs.at[0])
    loss_rows, grads = pairs()
    for h in range(L):
        ug_s[h] = scale * grads[h][T:]
    send(ug_s, ug_r, pair_ss.at[1], pair_rs.at[1], partner)
    arrived(ug_r, pair_rs.at[1])
    ug = [scale * grads[h][:T] + ug_r[h] for h in range(L)]
    inner = sum(jnp.sum(unit[h] * ug[h], axis=1, keepdims=True) for h in range(L))
    for h in range(L):
        mg_s[h] = ((ug[h] - unit[h] * inner) / length).astype(BF16)
    for o in range(1, X * L):
        other = lax.rem(x * L + y + o, X * L)
        send(
            mg_s.at[other % L], mga.at[rows(q, T)], mg_ss.at[o], mg_rs.at[q],
            ((other // L) * CORES + core, z * L + other % L),
        )
    send(mg_s.at[y], mga.at[rows(q, T)], mg_ss.at[0], mg_rs.at[q], partner)
    mga[rows(q, T)] = mg_s[y]
    for o in range(1, X * L):
        other = lax.rem(x * L + y + o, X * L)
        source = ((other // L) * CORES + core) * L + other % L
        at = mga.at[rows(source, T)]
        arrived(at, mg_rs.at[source])
        send(at, at, mg_ss.at[X * L + o], mg_rs.at[source], partner)
    for o in range(X * L):
        other = lax.rem(x * L + y + o, X * L)
        source = ((other // L) * CORES + 1 - core) * L + other % L
        arrived(mga.at[rows(source, T)], mg_rs.at[source])

    turned = mga[...].T

    def own_part(zd):
        gp[zd] = jnp.dot(turned[zd * Dp:(zd + 1) * Dp], hid[...], preferred_element_type=F32)

    def pass_on(zd, d, direction):
        first = z == (0 if d == 0 else Z - 1)
        before = z < zd if d == 0 else z > zd

        def add():
            arrived(gz.at[d, zd], g_rs.at[d, zd])
            gz_s[zd] = (gp[zd] + gz[d, zd].astype(F32)).astype(BF16)

        def start():
            gz_s[zd] = gp[zd].astype(BF16)

        pl.when(jnp.logical_and(before, first))(start)
        pl.when(jnp.logical_and(before, jnp.logical_not(first)))(add)
        send(
            gz_s.at[zd], gz.at[d, zd], g_ss.at[d, zd], g_rs.at[d, zd],
            (r, jnp.clip(z + direction, 0, Z - 1) * L + y), before,
        )

    for k in range(Z):
        up, down = Z - 1 - k, k
        if k < (Z + 1) // 2:
            own_part(up)
            if down != up:
                own_part(down)
        pass_on(up, 0, 1)
        pass_on(down, 1, -1)
    upd_ref[...] = gp[z][:Db]
    for d in range(2):
        def take():
            arrived(gz.at[d, z], g_rs.at[d, z])
            upd_ref[...] += gz[d, z][:Db].astype(F32)

        pl.when(z > 0 if d == 0 else z < Z - 1)(take)
    g = upd_ref[...]

    sq = g * g + FLOOR_VALUE
    rsb[r] = jnp.sum(sq, axis=1, keepdims=True)
    csb[c] = jnp.sum(sq, axis=0, keepdims=True)
    for o in range(1, C):
        c2 = lax.rem(c + o, C)
        send(csb.at[c], csb.at[c], col_ss.at[o], col_rs.at[c], (r, c2))
    for o in range(1, R):
        r2 = lax.rem(r + o, R)
        send(rsb.at[r], rsb.at[r], row_ss.at[o], row_rs.at[r], (r2, c))
    for o in range(1, R):
        r2 = lax.rem(r + o, R)
        arrived(rsb.at[r2], row_rs.at[r2])
    for o in range(1, C):
        c2 = lax.rem(c + o, C)
        arrived(csb.at[c2], col_rs.at[c2])
    row_sum = sum(rsb[k] for k in range(R))
    col_sum = sum(csb[k] for k in range(C))
    new_row = DECAY_RATE * rm_ref[...] + (1.0 - DECAY_RATE) * row_sum / (R * Fb)
    new_col = DECAY_RATE * cm_ref[...] + (1.0 - DECAY_RATE) * col_sum / (C * Db)
    nr_ref[...] = new_row
    nc_ref[...] = new_col
    raw = g / jnp.sqrt(new_row * new_col)
    upd_ref[...] = raw
    local = jnp.sum(jnp.sum(raw * raw, axis=1, keepdims=True), axis=0, keepdims=True)
    loss_local = jnp.sum(loss_rows, axis=0, keepdims=True)
    lane = lax.broadcasted_iota(jnp.int32, (1, 128), 1)
    me = r * C + c
    stb[me] = jnp.where(lane == 0, local, loss_local)

    def tell(o, wait):
        other = lax.rem(me + o, devices)
        copy = pltpu.make_async_remote_copy(
            src_ref=stb.at[me], dst_ref=stb.at[me], send_sem=st_ss.at[o], recv_sem=st_rs.at[me],
            device_id=(other // C, other % C), device_id_type=MESH,
        )
        if wait:
            copy.wait_send()
            arrived(stb.at[other], st_rs.at[other])
        else:
            copy.start()

    def tell_start(o, _):
        tell(o, False)
        return _

    def tell_wait(o, _):
        tell(o, True)
        return _

    lax.fori_loop(1, devices, tell_start, 0)
    lax.fori_loop(1, devices, tell_wait, 0)
    totals = jnp.sum(stb[...], axis=0)
    rms = jnp.sqrt(totals[:, 0:1] / (C * Db * R * Fb))
    upd_ref[...] = upd_ref[...] / jnp.maximum(1.0, rms / CLIP_LEVEL)
    loss_ref[...] = totals / batch
    for wait in finish:
        wait()


def per_device(pooled, hidden, text, weight, row_moment, col_moment, log_scale, bias):
    R, C = lax.axis_size("row"), lax.axis_size("col")
    L, X, Z = LOW, R // CORES, C // LOW
    T, D = pooled.shape
    Db, Fb = weight.shape
    Dp = -(-Db // 16) * 16
    F2 = Z * Dp
    plane = R * L
    texts = X * C * T
    chunk = min(texts, 512)

    def by_half(a):
        a = a.reshape(T, Z, L, Db).transpose(2, 0, 1, 3)
        if Dp != Db:
            a = jnp.pad(a, ((0, 0), (0, 0), (0, 0), (0, Dp - Db)))
        return a.reshape(L, T, F2)

    hs = hidden.reshape(T, R, Fb).transpose(1, 0, 2)
    wh = weight.astype(BF16)
    if Dp != Db:
        wh = jnp.pad(wh, ((0, Dp - Db), (0, 0)))
    tf = text.astype(F32)
    tn = (tf / jnp.sqrt(jnp.sum(tf * tf, axis=1, keepdims=True) + EPSILON)).astype(BF16)
    sizes = (R, C, X, Z, T, Db, Dp, Fb, chunk)
    vmem = pl.BlockSpec(memory_space=pltpu.VMEM)
    smem = pl.BlockSpec(memory_space=pltpu.SMEM)
    dma = lambda *s: pltpu.SemaphoreType.DMA(s)
    upd, nr, nc, loss = pl.pallas_call(
        functools.partial(kernel, sizes),
        out_shape=(
            jax.ShapeDtypeStruct((Db, Fb), F32),
            jax.ShapeDtypeStruct((Db, 1), F32),
            jax.ShapeDtypeStruct((1, Fb), F32),
            jax.ShapeDtypeStruct((1, 128), F32),
        ),
        in_specs=[vmem] * 6 + [smem] * 2,
        out_specs=(vmem,) * 4,
        scratch_shapes=[
            pltpu.VMEM((plane * T, Fb), BF16),
            pltpu.VMEM((F2, Fb), BF16),
            pltpu.VMEM((L, texts, F2), BF16),
            pltpu.VMEM((plane * T, F2), F32),
            pltpu.VMEM((X, L * T, F2), F32),
            pltpu.VMEM((X, L * T, F2), F32),
            pltpu.VMEM((X, L, T, F2), F32),
            pltpu.VMEM((L, T, F2), BF16),
            pltpu.VMEM((L, T, F2), BF16),
            pltpu.VMEM((L, T, F2), F32),
            pltpu.VMEM((L, T, F2), F32),
            pltpu.VMEM((L, T, F2), BF16),
            pltpu.VMEM((plane * T, F2), BF16),
            pltpu.VMEM((Z, Dp, Fb), F32),
            pltpu.VMEM((Z, Dp, Fb), BF16),
            pltpu.VMEM((2, Z, Dp, Fb), BF16),
            pltpu.VMEM((R, Db, 1), F32),
            pltpu.VMEM((C, 1, Fb), F32),
            pltpu.VMEM((R * C, 1, 128), F32),
            dma(plane), dma(plane), dma(2, Z), dma(Z), dma(2, Z), dma(2, Z, X + L), dma(X * C),
            dma(2, Z, X + L, X + L), dma(X * C, L), dma(X + 1), dma(X), dma(X * L + L), dma(X * L),
            dma(2), dma(2), dma(plane), dma(plane), dma(2, Z), dma(2, Z),
            dma(R), dma(R), dma(C), dma(C), dma(R * C), dma(R * C),
        ],
        compiler_params=pltpu.CompilerParams(
            has_side_effects=True, vmem_limit_bytes=60 * 1024 * 1024
        ),
    )(
        hs, wh, by_half(pooled), by_half(tn), row_moment[:, None], col_moment[None, :],
        log_scale[None], bias[None],
    )
    return upd, nr[:, 0], nc[0], loss[0, 1]


def solution(mesh):
    return jax.shard_map(
        per_device,
        mesh=mesh,
        in_specs=(
            P(("row", "col"), None),
            P(("row", "col"), None),
            P(("row", "col"), None),
            P("col", "row"),
            P("col"),
            P("row"),
            P(),
            P(),
        ),
        out_specs=(P("col", "row"), P("col"), P("row"), P()),
        check_vma=False,
    )
```
